32 devices in a mesh: groups: 2 (over y), expert: 4 (over z), dp: 2 (over core), tensor: 2 (over x).
Axes of the slice: x: 2, y: 2, z: 4, core: 2. Of those that a mesh axis runs over, the one named last changes fastest.
Arguments:
- tokens: bfloat16 [2, 2048, 2048], P('dp', ('groups', 'expert', 'tensor')), parts along dimension 1, may hold values from -6 to 6
- proj_weight: bfloat16 [4, 2048, 3584], P('expert', 'dp', 'tensor'), may hold values from -0.125 to 0.125
- slot_grads: bfloat16 [2, 4, 32, 3584], P('dp', 'expert', 'groups', 'tensor'), parts along dimension 2, may hold values from -1.5 to 1.5
- gate_weights: float32 [2, 2, 32], P('dp', None, 'groups'), parts along dimension 2, may hold values from 0.2 to 1
- selected: int32 [2, 2, 32], P('dp', None, 'groups'), parts along dimension 2, may hold values from 0 to 1023, as said below
Outputs:
- token_grads: bfloat16 [2, 2048, 2048], P('dp', ('groups', 'expert', 'tensor')), parts along dimension 1
- weight_grads: bfloat16 [8, 2048, 3584], P(('groups', 'expert'), 'dp', 'tensor'), parts along dimension 0
The draws below stay inside these ranges and needn't reach their ends.
There are 2 independent parts, one for each index of `groups`. The reference program is written for one: setup_inputs(seed, part) draws one part's arguments, and reference() takes and returns one part's arrays. A program takes and returns all parts, laid end to end along the dimension named above; an argument that names none is the same for every part. Nothing has to cross between parts.
Inputs may be any that keep to these rules, and one draw needn't show every extreme that they name: `selected`: each entry names a token of its own group. Within one group and one expert the 16 entries are distinct. In each group an expert takes at most 4 tokens from the 128 tokens of one device (tokens k * 128 to (k + 1) * 128 - 1), and exactly 4 from some devices.
All inputs are finite; a program needn't handle non-finite values.
Results may differ from the reference program's by a relative error of at most 0.011.
Values may be sent and summed in bfloat16 or wider, within the bound.
No kernel may reach another device: no remote copies, remote signals or barrier semaphores. Data moves between devices by JAX's collectives and lax.ppermute only.
A program may use at most 64 MiB of HBM per device.

```python
import math
import jax
import jax.numpy as jnp
from jax import lax

D = 2048
TOK_DEV = 128
MOST = 4
EXPERTS = 2
EXPERT_HALVES = 4
FFH = 3584
OWNERS = 8
CAP = 16
TOK_GROUP = 1024
DP_GROUPS = 2
N_TENSOR = 2


def draw_selected(key, part):

    def draw_group(group_key):
        key_order, sorted_key_rows, key_slots = jax.random.split(group_key, 3)
        owner_order = jax.random.permutation(key_order, OWNERS)
        full_owners = (CAP - OWNERS) // (MOST - 1)
        remainder = CAP - OWNERS - full_owners * (MOST - 1)
        positions = jnp.arange(OWNERS)
        count_rank = jnp.where(positions < full_owners, MOST, jnp.where(positions == full_owners, 1 + remainder, 1))
        counts = jnp.zeros((OWNERS,), jnp.int32).at[owner_order].set(count_rank.astype(jnp.int32))
        row_keys = jax.random.split(sorted_key_rows, OWNERS)
        row_order = jax.vmap(lambda row_key: jax.random.permutation(row_key, TOK_DEV)[:MOST])(row_keys)
        candidates = jnp.arange(OWNERS)[:, None] * TOK_DEV + row_order
        within = jnp.arange(MOST)[None, :] < counts[:, None]
        priority = jnp.arange(OWNERS * MOST) + jnp.where(within, 0, OWNERS * MOST).reshape(-1)
        order = jnp.argsort(priority, stable=True)[:CAP]
        chosen = candidates.reshape(-1)[order]
        return chosen[jax.random.permutation(key_slots, CAP)]
    group_keys = jax.random.split(jax.random.fold_in(key, 7), DP_GROUPS * EXPERTS)
    drawn = jax.vmap(draw_group)(group_keys)
    return drawn.reshape(DP_GROUPS, EXPERTS, CAP).astype(jnp.int32)


def block_levels(key, dims, pieces, low, top_value):
    factor_of = 1.0
    for dim, parts in pieces:
        heights = jax.random.uniform(jax.random.fold_in(jax.random.fold_in(key, 6), dim), (parts,), jnp.float32, low / len(pieces), top_value / len(pieces))
        factor_of = factor_of * jnp.repeat(jnp.exp(heights), dims[dim] // parts).reshape((-1,) + (1,) * (len(dims) - 1 - dim))
    return factor_of


def noise(stream_key, extent, scale, limit, cuts=(), dtype=jnp.bfloat16):
    factor_of = block_levels(stream_key, extent, cuts, -0.22, 0.18) if cuts else 1.0
    values = jax.random.normal(stream_key, extent, jnp.float32) * scale * factor_of
    return jnp.minimum(jnp.maximum(values, -limit), limit).astype(dtype)


def setup_inputs(seed: int = 0, part: int = 0) -> dict:
    arg_keys = jax.random.split(jax.random.key(seed), 6)
    part_keys = jax.random.split(jax.random.fold_in(arg_keys[5], part), 6)
    return {
        "tokens": noise(part_keys[0], (DP_GROUPS, TOK_GROUP, D), 1.0, 6.0, ((0, 2), (1, 8))),
        "proj_weight": noise(arg_keys[1], (EXPERT_HALVES, D, FFH), D ** -0.5, 0.125, ((0, 4), (1, 2), (2, 2))),
        "slot_grads": noise(part_keys[2], (DP_GROUPS, EXPERT_HALVES, CAP, FFH), 0.25, 1.5, ((0, 2), (1, 4), (3, 2))),
        "gate_weights": jnp.clip(jnp.exp(math.log(1.0) - 1.609438 * jax.random.uniform(part_keys[3], (DP_GROUPS, EXPERTS, CAP), jnp.float32) ** block_levels(part_keys[3], (DP_GROUPS, EXPERTS, CAP), ((0, 2),), -0.2, 0.2)), 0.2, 1.0),
        "selected": draw_selected(jax.random.fold_in(jax.random.fold_in(arg_keys[5], part), 71), part),
    }


def gated_slots(group_gate_values, grads_group, half_index):
    expert_index = half_index // 2
    gate_row = lax.dynamic_index_in_dim(group_gate_values, expert_index, 0, keepdims=False)
    grad_block = lax.dynamic_index_in_dim(grads_group, half_index, 0, keepdims=False)
    return (gate_row[:, None] * grad_block.astype(jnp.float32)).astype(jnp.bfloat16)


def reference(tokens, proj_weight, slot_grads, gate_weights, selected):
    group_count = tokens.shape[0]
    half_count = proj_weight.shape[0]
    features = proj_weight.shape[1]
    hidden = proj_weight.shape[2]
    block = hidden // N_TENSOR
    capacity = selected.shape[2]
    token_list = []
    for group in range(group_count):
        def step(carry, half_index):
            chosen = lax.dynamic_index_in_dim(selected[group], half_index // 2, 0, keepdims=False)
            scaled = gated_slots(gate_weights[group], slot_grads[group], half_index)
            block_list = scaled.astype(jnp.float32).reshape(capacity, N_TENSOR, block)
            input_weight = lax.dynamic_index_in_dim(proj_weight, half_index, 0, keepdims=False)
            input_weight = input_weight.astype(jnp.float32).reshape(features, N_TENSOR, block)
            partial_value_sum = jnp.einsum("lki,xki->lkx", block_list, input_weight).astype(jnp.bfloat16).astype(jnp.float32)
            return carry.at[chosen].add(jnp.sum(partial_value_sum, axis=1)), None

        start = jnp.zeros((tokens.shape[1], features), jnp.float32)
        total, _ = lax.scan(step, start, jnp.arange(half_count).astype(jnp.int32))
        token_list.append(total.astype(jnp.bfloat16))
    token_grads = jnp.stack(token_list, axis=0)

    def per_half(half_index):
        total = jnp.zeros((features, hidden), jnp.float32)
        for group in range(group_count):
            chosen = lax.dynamic_index_in_dim(selected[group], half_index // 2, 0, keepdims=False)
            gathered = tokens[group][chosen]
            scaled = gated_slots(gate_weights[group], slot_grads[group], half_index)
            term = jnp.dot(gathered.T, scaled, preferred_element_type=jnp.float32)
            total = total + term.astype(jnp.bfloat16).astype(jnp.float32)
        return total.astype(jnp.bfloat16)

    weight_grads = lax.map(per_half, jnp.arange(half_count).astype(jnp.int32))
    return token_grads, weight_grads
```

```python
import functools

import jax
import jax.numpy as jnp
from jax import lax
from jax.experimental import pallas as pl
from jax.experimental.pallas import tpu as pltpu
from jax.sharding import PartitionSpec as P

MOST = 4
BF16 = jnp.bfloat16
F32 = jnp.float32
VMEM = pl.BlockSpec(memory_space=pltpu.VMEM)


def params(limit_mib=24):
    return pltpu.CompilerParams(vmem_limit_bytes=limit_mib * 2**20)


def to_column(row):
    n = row.shape[1]
    eye = lax.broadcasted_iota(jnp.int32, (n, n), 0) == lax.broadcasted_iota(jnp.int32, (n, n), 1)
    return jnp.sum(jnp.where(eye, row, jnp.zeros_like(row)), axis=1, keepdims=True)


def owner_and_arrival(chosen, tok_dev):
    n = chosen.shape[1]
    owner = chosen // tok_dev
    before = lax.broadcasted_iota(jnp.int32, (n, n), 0) < lax.broadcasted_iota(jnp.int32, (n, n), 1)
    same = to_column(owner) == owner
    arrival = jnp.sum(jnp.where(same & before, 1, 0), axis=0, keepdims=True)
    return owner, arrival


def own_rows(chosen_ref, owner_id, tok_dev):
    out = []
    for e in range(chosen_ref.shape[0]):
        chosen = chosen_ref[e : e + 1, :]
        owner, arrival = owner_and_arrival(chosen, tok_dev)
        place = jnp.where(owner == owner_id, arrival, -1)
        hit = lax.broadcasted_iota(jnp.int32, (MOST, chosen.shape[1]), 0) == place
        out.append(jnp.sum(jnp.where(hit, chosen - owner * tok_dev + 1, 0), axis=1, keepdims=True))
    return jnp.concatenate(out, axis=0)


def prep_kernel(n_expert, n_tensor, n_data, chosen_ref, gate_ref, grads_ref, tokens_ref, send_ref, scaled_ref):
    tok_dev, features = tokens_ref.shape
    experts = chosen_ref.shape[0]
    halves = n_expert // experts
    share = features // n_data
    own_half = lax.axis_index("expert")
    owner_id = own_half * n_tensor + lax.axis_index("tensor")
    target = own_rows(chosen_ref, owner_id, tok_dev)
    onehot = (lax.broadcasted_iota(jnp.int32, (experts * MOST, tok_dev), 1) + 1 == target).astype(F32).astype(BF16)
    rows = jnp.dot(onehot, tokens_ref[...], preferred_element_type=F32)
    for e in range(experts):
        block = rows[e * MOST : (e + 1) * MOST].astype(BF16)
        for d in range(n_data):
            piece = block[:, d * share : (d + 1) * share]
            for k in range(halves * n_tensor):
                send_ref[(d * experts + e) * halves * n_tensor + k] = piece
    own_expert = own_half // halves
    chosen = chosen_ref[pl.ds(own_expert, 1), :]
    owner, arrival = owner_and_arrival(chosen, tok_dev)
    places = n_expert * n_tensor * MOST
    capacity = chosen.shape[1]
    spread = lax.broadcasted_iota(jnp.int32, (places, capacity), 0) == owner * MOST + arrival
    gate = to_column(gate_ref[pl.ds(own_expert, 1), :])
    scaled = (gate * grads_ref[...].astype(F32)).astype(BF16)
    scaled_ref[...] = jnp.dot(spread.astype(F32).astype(BF16), scaled, preferred_element_type=F32).astype(BF16)


def partial_kernel(own_ref, other_ref, weight_ref, part_ref, all_ref):
    places = own_ref.shape[0]
    group = lax.axis_index("dp")
    all_ref[pl.ds(pl.multiple_of(group * places, places), places), :] = own_ref[...]
    all_ref[pl.ds(pl.multiple_of((1 - group) * places, places), places), :] = other_ref[...]
    part = lax.dot_general(
        all_ref[...], weight_ref[...], (((1,), (1,)), ((), ())), preferred_element_type=F32
    )
    part_ref[...] = part.astype(BF16)


def weight_kernel(rows_ref, scaled_ref, out_ref):
    out_ref[...] = lax.dot_general(
        rows_ref[...], scaled_ref[...], (((0,), (0,)), ((), ())), preferred_element_type=F32
    ).astype(BF16)


def token_kernel(n_expert, n_tensor, n_data, chosen_ref, parts_ref, out_ref):
    tok_dev, features = out_ref.shape
    experts = chosen_ref.shape[0]
    halves = n_expert // experts
    share = features // n_data
    owner_id = lax.axis_index("expert") * n_tensor + lax.axis_index("tensor")
    target = own_rows(chosen_ref, owner_id, tok_dev)
    wide = jnp.concatenate(
        [target[e * MOST : (e + 1) * MOST] for e in range(experts) for _ in range(halves * n_tensor)], axis=0
    )
    places = wide.shape[0]
    onehot = (lax.broadcasted_iota(jnp.int32, (places, tok_dev), 1) + 1 == wide).astype(F32).astype(BF16)
    for d in range(n_data):
        out_ref[:, d * share : (d + 1) * share] = lax.dot_general(
            onehot,
            parts_ref[d * places : (d + 1) * places, :],
            (((0,), (0,)), ((), ())),
            preferred_element_type=F32,
        ).astype(BF16)


def exchange(blocks):
    return lax.all_to_all(blocks, ("dp", "expert", "tensor"), split_axis=0, concat_axis=0, tiled=True)


def local(tokens, proj_weight, slot_grads, gate_weights, selected):
    n_tensor = lax.axis_size("tensor")
    n_expert = lax.axis_size("expert")
    n_data = lax.axis_size("dp")
    sizes = (n_expert, n_tensor, n_data)
    members = n_expert * n_tensor * n_data
    places = n_expert * n_tensor * MOST
    tok_dev, features = tokens.shape[1:]
    hidden = proj_weight.shape[2]
    share = features // n_data
    send, own = pl.pallas_call(
        functools.partial(prep_kernel, *sizes),
        out_shape=(
            jax.ShapeDtypeStruct((members, MOST, share), BF16),
            jax.ShapeDtypeStruct((places, hidden), BF16),
        ),
        in_specs=[VMEM] * 4,
        out_specs=(VMEM, VMEM),
        compiler_params=params(),
        cost_estimate=pl.CostEstimate(flops=10**8, bytes_accessed=10**6, transcendentals=0),
        name="prep",
    )(selected[0], gate_weights[0], slot_grads[0, 0], tokens[0])
    other = lax.ppermute(own, "dp", [(0, 1), (1, 0)])
    arrived = exchange(send)
    part, scaled = pl.pallas_call(
        partial_kernel,
        out_shape=(
            jax.ShapeDtypeStruct((n_data * places, share), BF16),
            jax.ShapeDtypeStruct((n_data * places, hidden), BF16),
        ),
        in_specs=[VMEM] * 3,
        out_specs=(VMEM, VMEM),
        compiler_params=params(),
        cost_estimate=pl.CostEstimate(flops=10**9, bytes_accessed=4 * 10**6, transcendentals=0),
        name="partial",
    )(own, other, proj_weight[0])
    returned = exchange(part.reshape(members, MOST, share))
    rows = arrived.reshape(n_data * places, share)
    block = min(256, share)
    weight_grads = pl.pallas_call(
        weight_kernel,
        grid=(share // block,),
        out_shape=jax.ShapeDtypeStruct((share, hidden), BF16),
        in_specs=[
            pl.BlockSpec((n_data * places, block), lambda i: (0, i)),
            pl.BlockSpec((n_data * places, hidden), lambda i: (0, 0)),
        ],
        out_specs=pl.BlockSpec((block, hidden), lambda i: (i, 0)),
        compiler_params=params(),
        cost_estimate=pl.CostEstimate(flops=10**9, bytes_accessed=4 * 10**6, transcendentals=0),
        name="weight_grad",
    )(rows, scaled)
    token_grads = pl.pallas_call(
        functools.partial(token_kernel, *sizes),
        out_shape=jax.ShapeDtypeStruct((tok_dev, features), BF16),
        in_specs=[VMEM] * 2,
        out_specs=VMEM,
        compiler_params=params(),
        cost_estimate=pl.CostEstimate(flops=10**8, bytes_accessed=10**6, transcendentals=0),
        name="token_grad",
    )(selected[0], returned.reshape(n_data * places, share))
    return token_grads[None], weight_grads[None]


def solution(mesh):
    in_specs = (
        P("dp", ("groups", "expert", "tensor"), None),
        P("expert", "dp", "tensor"),
        P("dp", "expert", "groups", "tensor"),
        P("dp", None, "groups"),
        P("dp", None, "groups"),
    )
    out_specs = (
        P("dp", ("groups", "expert", "tensor"), None),
        P(("groups", "expert"), "dp", "tensor"),
    )
    return jax.shard_map(local, mesh=mesh, in_specs=in_specs, out_specs=out_specs, check_vma=False)
```

```python
import functools

import jax
import jax.numpy as jnp
from jax import lax
from jax.experimental import pallas as pl
from jax.experimental.pallas import tpu as pltpu
from jax.sharding import PartitionSpec as P

MOST = 4
BLOCK = 2 * MOST
BF16 = jnp.bfloat16
F32 = jnp.float32
VMEM = pl.BlockSpec(memory_space=pltpu.VMEM)
HBM = pl.BlockSpec(memory_space=pltpu.HBM)
DMA = pltpu.SemaphoreType.DMA


def params(limit_mib=24):
    return pltpu.CompilerParams(vmem_limit_bytes=limit_mib * 2**20)


def cost(flops, moved):
    return pl.CostEstimate(flops=flops, bytes_accessed=moved, transcendentals=0)


def to_column(row):
    n = row.shape[1]
    eye = lax.broadcasted_iota(jnp.int32, (n, n), 0) == lax.broadcasted_iota(jnp.int32, (n, n), 1)
    return jnp.sum(jnp.where(eye, row, jnp.zeros_like(row)), axis=1, keepdims=True)


def owner_and_arrival(chosen, tok_dev):
    n = chosen.shape[1]
    owner = chosen // tok_dev
    before = lax.broadcasted_iota(jnp.int32, (n, n), 0) < lax.broadcasted_iota(jnp.int32, (n, n), 1)
    same = to_column(owner) == owner
    arrival = jnp.sum(jnp.where(same & before, 1, 0), axis=0, keepdims=True)
    return owner, arrival


def own_rows(chosen_ref, owner_id, tok_dev):
    out = []
    for e in range(chosen_ref.shape[0]):
        chosen = chosen_ref[e : e + 1, :]
        owner, arrival = owner_and_arrival(chosen, tok_dev)
        place = jnp.where(owner == owner_id, arrival, -1)
        hit = lax.broadcasted_iota(jnp.int32, (MOST, chosen.shape[1]), 0) == place
        out.append(jnp.sum(jnp.where(hit, chosen - owner * tok_dev + 1, 0), axis=1, keepdims=True))
    return out


def as_onehot(mask):
    return mask.astype(F32).astype(BF16)


def spread(chosen, owners, tok_dev, offset):
    owner, arrival = owner_and_arrival(chosen, tok_dev)
    shape = (owners * BLOCK, chosen.shape[1])
    return as_onehot(lax.broadcasted_iota(jnp.int32, shape, 0) == owner * BLOCK + arrival + offset)


def gated(gate_row, grads):
    return (to_column(gate_row) * grads.astype(F32)).astype(BF16)


def prep_kernel(
    n_expert,
    n_tensor,
    n_data,
    chosen_hbm,
    gate_hbm,
    grads_hbm,
    tokens_hbm,
    weight_hbm,
    weight_ref,
    send_ref,
    scaled_ref,
    placed_ref,
    spread_ref,
    hits_ref,
    chosen_ref,
    gate_ref,
    grads_ref,
    tokens_ref,
    sems,
):
    loads = [
        pltpu.make_async_copy(src, dst, sems.at[i])
        for i, (src, dst) in enumerate(
            (
                (chosen_hbm, chosen_ref),
                (gate_hbm, gate_ref),
                (grads_hbm, grads_ref),
                (tokens_hbm, tokens_ref),
                (weight_hbm, weight_ref),
            )
        )
    ]
    for load in loads:
        load.start()
    tok_dev, features = tokens_ref.shape
    experts = chosen_ref.shape[0]
    halves = n_expert // experts
    owners = n_expert * n_tensor
    share = features // n_data
    own_half = lax.axis_index("expert")
    owner_id = own_half * n_tensor + lax.axis_index("tensor")
    own_expert = own_half // halves
    loads[0].wait()
    target = own_rows(chosen_ref, owner_id, tok_dev)
    empty = jnp.zeros((MOST, 1), jnp.int32)
    outgoing = jnp.concatenate([t for e in range(experts) for t in (target[e], empty) * (halves * n_tensor)], axis=0)
    incoming = jnp.concatenate([t for e in range(experts) for t in (empty, target[e]) * (halves * n_tensor)], axis=0)
    rows = lax.broadcasted_iota(jnp.int32, (owners * BLOCK, tok_dev), 1) + 1
    hits_ref[...] = as_onehot(rows == incoming)
    pick = as_onehot(rows == outgoing)
    chosen = chosen_ref[pl.ds(own_expert, 1), :]
    spread_ref[...] = spread(chosen, owners, tok_dev, MOST)
    loads[1].wait()
    loads[2].wait()
    scaled = gated(gate_ref[pl.ds(own_expert, 1), :], grads_ref[...])
    scaled_ref[...] = scaled
    placed_ref[...] = jnp.dot(
        spread(chosen, owners, tok_dev, 0), scaled, preferred_element_type=F32
    ).astype(BF16)
    loads[3].wait()
    for d in range(n_data):
        send_ref[d * owners * BLOCK : (d + 1) * owners * BLOCK, :] = jnp.dot(
            pick, tokens_ref[:, d * share : (d + 1) * share], preferred_element_type=F32
        ).astype(BF16)
    loads[4].wait()


def partial_kernel(
    n_expert,
    n_tensor,
    tok_dev,
    chosen_ref,
    gate_ref,
    grads_ref,
    weight_ref,
    rows_ref,
    scaled_ref,
    placed_ref,
    spread_ref,
    send_ref,
    all_ref,
):
    owners = n_expert * n_tensor
    places = owners * BLOCK
    halves = n_expert // chosen_ref.shape[0]
    capacity = chosen_ref.shape[1]
    own_expert = lax.axis_index("expert") // halves
    group = lax.axis_index("dp")
    mine = pl.ds(pl.multiple_of(group * places, places), places)
    theirs = pl.ds(pl.multiple_of((1 - group) * places, places), places)
    chosen = chosen_ref[pl.ds(own_expert, 1), :]
    scaled = gated(gate_ref[pl.ds(own_expert, 1), :], grads_ref[...])
    part = lax.dot_general(
        jnp.concatenate([scaled_ref[...], scaled], axis=0),
        weight_ref[...],
        (((1,), (1,)), ((), ())),
        preferred_element_type=F32,
    ).astype(BF16)
    put = spread(chosen, owners, tok_dev, MOST)
    for where, place, piece in ((mine, spread_ref[...], part[:capacity]), (theirs, put, part[capacity:])):
        out = jnp.dot(place, piece, preferred_element_type=F32)
        send_ref[where, :] = (out + rows_ref[where, :].astype(F32)).astype(BF16)
    all_ref[mine, :] = placed_ref[...]
    all_ref[theirs, :] = jnp.dot(
        spread(chosen, owners, tok_dev, 0), scaled, preferred_element_type=F32
    ).astype(BF16)


def finish_kernel(
    n_data, chunk, arrived_ref, scaled_ref, hits_ref, weight_hbm, token_hbm, weight_buf, token_buf, weight_sems, token_sem
):
    share, hidden = weight_hbm.shape
    places = hits_ref.shape[0]
    stores = []
    for i in range(share // chunk):
        here = slice(i * chunk, (i + 1) * chunk)
        weight_buf[here, :] = lax.dot_general(
            arrived_ref[:, here], scaled_ref[...], (((0,), (0,)), ((), ())), preferred_element_type=F32
        ).astype(BF16)
        stores.append(pltpu.make_async_copy(weight_buf.at[here, :], weight_hbm.at[here, :], weight_sems.at[i]))
        stores[-1].start()
    for d in range(n_data):
        token_buf[:, d * share : (d + 1) * share] = lax.dot_general(
            hits_ref[...],
            arrived_ref[d * places : (d + 1) * places, :],
            (((0,), (0,)), ((), ())),
            preferred_element_type=F32,
        ).astype(BF16)
    stores.append(pltpu.make_async_copy(token_buf, token_hbm, token_sem))
    stores[-1].start()
    for store in stores:
        store.wait()


def local(tokens, proj_weight, slot_grads, gate_weights, selected):
    n_tensor = lax.axis_size("tensor")
    n_expert = lax.axis_size("expert")
    n_data = lax.axis_size("dp")
    owners = n_expert * n_tensor
    members = owners * n_data
    places = owners * BLOCK
    tok_dev, features = tokens.shape[1:]
    hidden = proj_weight.shape[2]
    experts, capacity = selected.shape[1:]
    share = features // n_data
    chosen, gate, grads = selected[0], gate_weights[0], slot_grads[0, 0]
    swap = [(0, 1), (1, 0)]
    other_grads = lax.ppermute(grads, "dp", swap)
    other_chosen = lax.ppermute(chosen, "dp", swap)
    other_gate = lax.ppermute(gate, "dp", swap)
    weight, rows, scaled, placed, spread_own, hits = pl.pallas_call(
        functools.partial(prep_kernel, n_expert, n_tensor, n_data),
        out_shape=(
            jax.ShapeDtypeStruct((share, hidden), BF16),
            jax.ShapeDtypeStruct((n_data * places, share), BF16),
            jax.ShapeDtypeStruct((capacity, hidden), BF16),
            jax.ShapeDtypeStruct((places, hidden), BF16),
            jax.ShapeDtypeStruct((places, capacity), BF16),
            jax.ShapeDtypeStruct((places, tok_dev), BF16),
        ),
        in_specs=[HBM] * 5,
        out_specs=(VMEM,) * 6,
        scratch_shapes=[
            pltpu.VMEM((experts, capacity), jnp.int32),
            pltpu.VMEM((experts, capacity), F32),
            pltpu.VMEM((capacity, hidden), BF16),
            pltpu.VMEM((tok_dev, features), BF16),
            DMA((5,)),
        ],
        compiler_params=params(),
        cost_estimate=cost(10**8, 5 * 10**6),
        name="prep",
    )(*(pltpu.with_memory_space_constraint(x, pltpu.HBM) for x in (chosen, gate, grads, tokens[0], proj_weight[0])))
    send, scaled_all = pl.pallas_call(
        functools.partial(partial_kernel, n_expert, n_tensor, tok_dev),
        out_shape=(
            jax.ShapeDtypeStruct((n_data * places, share), BF16),
            jax.ShapeDtypeStruct((n_data * places, hidden), BF16),
        ),
        in_specs=[VMEM] * 8,
        out_specs=(VMEM, VMEM),
        compiler_params=params(),
        cost_estimate=cost(10**9, 4 * 10**6),
        name="partial",
    )(other_chosen, other_gate, other_grads, weight, rows, scaled, placed, spread_own)
    arrived = lax.all_to_all(
        send.reshape(members, BLOCK, share), ("dp", "expert", "tensor"), split_axis=0, concat_axis=0, tiled=True
    )
    chunk = min(128, share)
    weight_grads, token_grads = pl.pallas_call(
        functools.partial(finish_kernel, n_data, chunk),
        out_shape=(
            jax.ShapeDtypeStruct((share, hidden), BF16),
            jax.ShapeDtypeStruct((tok_dev, features), BF16),
        ),
        in_specs=[VMEM] * 3,
        out_specs=(HBM, HBM),
        scratch_shapes=[
            pltpu.VMEM((share, hidden), BF16),
            pltpu.VMEM((tok_dev, features), BF16),
            DMA((share // chunk,)),
            DMA,
        ],
        compiler_params=params(),
        cost_estimate=cost(10**9, 4 * 10**6),
        name="finish",
    )(arrived.reshape(n_data * places, share), scaled_all, hits)
    return token_grads[None], weight_grads[None]


def solution(mesh):
    in_specs = (
        P("dp", ("groups", "expert", "tensor"), None),
        P("expert", "dp", "tensor"),
        P("dp", "expert", "groups", "tensor"),
        P("dp", None, "groups"),
        P("dp", None, "groups"),
    )
    out_specs = (
        P("dp", ("groups", "expert", "tensor"), None),
        P(("groups", "expert"), "dp", "tensor"),
    )
    return jax.shard_map(local, mesh=mesh, in_specs=in_specs, out_specs=out_specs, check_vma=False)
```

```python
import functools

import jax
import jax.numpy as jnp
from jax import lax
from jax.experimental import pallas as pl
from jax.experimental.pallas import tpu as pltpu
from jax.sharding import PartitionSpec as P

MOST = 4
BLOCK = 2 * MOST
BF16 = jnp.bfloat16
F32 = jnp.float32
VMEM = pl.BlockSpec(memory_space=pltpu.VMEM)
HBM = pl.BlockSpec(memory_space=pltpu.HBM)
DMA = pltpu.SemaphoreType.DMA


def params(limit_mib=24):
    return pltpu.CompilerParams(vmem_limit_bytes=limit_mib * 2**20)


def cost(flops, moved):
    return pl.CostEstimate(flops=flops, bytes_accessed=moved, transcendentals=0)


def to_column(row):
    n = row.shape[1]
    eye = lax.broadcasted_iota(jnp.int32, (n, n), 0) == lax.broadcasted_iota(jnp.int32, (n, n), 1)
    return jnp.sum(jnp.where(eye, row, jnp.zeros_like(row)), axis=1, keepdims=True)


def owner_and_arrival(chosen, tok_dev):
    n = chosen.shape[1]
    owner = chosen // tok_dev
    before = lax.broadcasted_iota(jnp.int32, (n, n), 0) < lax.broadcasted_iota(jnp.int32, (n, n), 1)
    same = to_column(owner) == owner
    arrival = jnp.sum(jnp.where(same & before, 1, 0), axis=0, keepdims=True)
    return owner, arrival


def own_places(chosen_ref, gate_ref, owner_id, tok_dev):
    targets, gates = [], []
    for e in range(chosen_ref.shape[0]):
        chosen = chosen_ref[e : e + 1, :]
        owner, arrival = owner_and_arrival(chosen, tok_dev)
        place = jnp.where(owner == owner_id, arrival, -1)
        hit = lax.broadcasted_iota(jnp.int32, (MOST, chosen.shape[1]), 0) == place
        targets.append(jnp.sum(jnp.where(hit, chosen - owner * tok_dev + 1, 0), axis=1, keepdims=True))
        gates.append(jnp.sum(jnp.where(hit, gate_ref[e : e + 1, :], 0.0), axis=1, keepdims=True))
    return targets, gates


def as_onehot(mask):
    return mask.astype(F32).astype(BF16)


def spread(chosen, owners, tok_dev, offset):
    owner, arrival = owner_and_arrival(chosen, tok_dev)
    shape = (owners * BLOCK, chosen.shape[1])
    return as_onehot(lax.broadcasted_iota(jnp.int32, shape, 0) == owner * BLOCK + arrival + offset)


def prep_kernel(
    n_expert,
    n_tensor,
    n_data,
    chosen_hbm,
    gate_hbm,
    grads_hbm,
    tokens_hbm,
    send_ref,
    grads_ref,
    placed_ref,
    spread_ref,
    hits_ref,
    chosen_ref,
    gate_ref,
    tokens_ref,
    sems,
):
    pairs = (
        (chosen_hbm, chosen_ref),
        (gate_hbm, gate_ref),
        (grads_hbm, grads_ref),
        (tokens_hbm, tokens_ref),
    )
    loads = [pltpu.make_async_copy(src, dst, sems.at[i]) for i, (src, dst) in enumerate(pairs)]
    for load in loads:
        load.start()
    tok_dev, features = tokens_ref.shape
    experts = chosen_ref.shape[0]
    halves = n_expert // experts
    owners = n_expert * n_tensor
    places = owners * BLOCK
    share = features // n_data
    own_half = lax.axis_index("expert")
    owner_id = own_half * n_tensor + lax.axis_index("tensor")
    own_expert = own_half // halves
    loads[0].wait()
    loads[1].wait()
    targets, gates = own_places(chosen_ref, gate_ref, owner_id, tok_dev)

    def column(pieces, first):
        none = jnp.zeros_like(pieces[0])
        both = [(p, none) if first else (none, p) for p in pieces]
        return jnp.concatenate([t for pair in both for t in pair * (halves * n_tensor)], axis=0)

    rows = lax.broadcasted_iota(jnp.int32, (places, tok_dev), 1) + 1
    weighted = jnp.where(rows == column(targets, False), column(gates, False), 0.0)
    high = weighted.astype(BF16)
    hits_ref[:places, :] = high
    hits_ref[places:, :] = (weighted - high.astype(F32)).astype(BF16)
    pick = as_onehot(rows == column(targets, True))
    gate = column(gates, True)
    chosen = chosen_ref[pl.ds(own_expert, 1), :]
    spread_ref[...] = spread(chosen, owners, tok_dev, MOST)
    loads[2].wait()
    placed_ref[...] = jnp.dot(
        spread(chosen, owners, tok_dev, 0), grads_ref[...], preferred_element_type=F32
    ).astype(BF16)
    loads[3].wait()
    for d in range(n_data):
        picked = jnp.dot(pick, tokens_ref[:, d * share : (d + 1) * share], preferred_element_type=F32)
        send_ref[d * places : (d + 1) * places, :] = (gate * picked).astype(BF16)


def partial_kernel(
    n_expert,
    n_tensor,
    tok_dev,
    chosen_ref,
    other_ref,
    weight_ref,
    rows_ref,
    grads_ref,
    placed_ref,
    spread_ref,
    send_ref,
    all_ref,
):
    owners = n_expert * n_tensor
    places = owners * BLOCK
    halves = n_expert // chosen_ref.shape[0]
    capacity = chosen_ref.shape[1]
    own_expert = lax.axis_index("expert") // halves
    group = lax.axis_index("dp")
    mine = pl.ds(pl.multiple_of(group * places, places), places)
    theirs = pl.ds(pl.multiple_of((1 - group) * places, places), places)
    chosen = chosen_ref[pl.ds(own_expert, 1), :]
    other = other_ref[...]
    part = lax.dot_general(
        jnp.concatenate([grads_ref[...], other], axis=0),
        weight_ref[...],
        (((1,), (1,)), ((), ())),
        preferred_element_type=F32,
    ).astype(BF16)
    put = spread(chosen, owners, tok_dev, MOST)
    for where, place, piece in ((mine, spread_ref[...], part[:capacity]), (theirs, put, part[capacity:])):
        out = jnp.dot(place, piece, preferred_element_type=F32)
        send_ref[where, :] = (out + rows_ref[where, :].astype(F32)).astype(BF16)
    all_ref[mine, :] = placed_ref[...]
    all_ref[theirs, :] = jnp.dot(
        spread(chosen, owners, tok_dev, 0), other, preferred_element_type=F32
    ).astype(BF16)


def finish_kernel(
    n_data, chunk, arrived_ref, scaled_ref, hits_ref, weight_hbm, token_hbm, weight_buf, token_buf, weight_sems, token_sem
):
    share, hidden = weight_hbm.shape
    places = hits_ref.shape[0] // 2
    stores = []
    for i in range(share // chunk):
        here = slice(i * chunk, (i + 1) * chunk)
        weight_buf[here, :] = lax.dot_general(
            arrived_ref[:, here], scaled_ref[...], (((0,), (0,)), ((), ())), preferred_element_type=F32
        ).astype(BF16)
        stores.append(pltpu.make_async_copy(weight_buf.at[here, :], weight_hbm.at[here, :], weight_sems.at[i]))
        stores[-1].start()
    for d in range(n_data):
        piece = arrived_ref[d * places : (d + 1) * places, :]
        total = sum(
            lax.dot_general(hits, piece, (((0,), (0,)), ((), ())), preferred_element_type=F32)
            for hits in (hits_ref[:places, :], hits_ref[places:, :])
        )
        token_buf[:, d * share : (d + 1) * share] = total.astype(BF16)
    stores.append(pltpu.make_async_copy(token_buf, token_hbm, token_sem))
    stores[-1].start()
    for store in stores:
        store.wait()


def local(tokens, proj_weight, slot_grads, gate_weights, selected):
    n_tensor = lax.axis_size("tensor")
    n_expert = lax.axis_size("expert")
    n_data = lax.axis_size("dp")
    owners = n_expert * n_tensor
    members = owners * n_data
    places = owners * BLOCK
    tok_dev, features = tokens.shape[1:]
    hidden = proj_weight.shape[2]
    experts, capacity = selected.shape[1:]
    share = features // n_data
    chosen, gate, grads = selected[0], gate_weights[0], slot_grads[0, 0]
    swap = [(0, 1), (1, 0)]
    other_grads = lax.ppermute(grads, "dp", swap)
    other_chosen = lax.ppermute(chosen, "dp", swap)
    rows, own_grads, placed, spread_own, hits = pl.pallas_call(
        functools.partial(prep_kernel, n_expert, n_tensor, n_data),
        out_shape=(
            jax.ShapeDtypeStruct((n_data * places, share), BF16),
            jax.ShapeDtypeStruct((capacity, hidden), BF16),
            jax.ShapeDtypeStruct((places, hidden), BF16),
            jax.ShapeDtypeStruct((places, capacity), BF16),
            jax.ShapeDtypeStruct((2 * places, tok_dev), BF16),
        ),
        in_specs=[HBM] * 4,
        out_specs=(VMEM,) * 5,
        scratch_shapes=[
            pltpu.VMEM((experts, capacity), jnp.int32),
            pltpu.VMEM((experts, capacity), F32),
            pltpu.VMEM((tok_dev, features), BF16),
            DMA((4,)),
        ],
        compiler_params=params(),
        cost_estimate=cost(12 * 10**8, 10**6),
        name="prep",
    )(*(pltpu.with_memory_space_constraint(x, pltpu.HBM) for x in (chosen, gate, grads, tokens[0])))
    send, scaled_all = pl.pallas_call(
        functools.partial(partial_kernel, n_expert, n_tensor, tok_dev),
        out_shape=(
            jax.ShapeDtypeStruct((n_data * places, share), BF16),
            jax.ShapeDtypeStruct((n_data * places, hidden), BF16),
        ),
        in_specs=[VMEM] * 7,
        out_specs=(VMEM, VMEM),
        compiler_params=params(),
        cost_estimate=cost(10**9, 4 * 10**6),
        name="partial",
    )(other_chosen, other_grads, proj_weight[0], rows, own_grads, placed, spread_own)
    arrived = lax.all_to_all(
        send.reshape(members, BLOCK, share), ("dp", "expert", "tensor"), split_axis=0, concat_axis=0, tiled=True
    )
    chunk = min(128, share)
    weight_grads, token_grads = pl.pallas_call(
        functools.partial(finish_kernel, n_data, chunk),
        out_shape=(
            jax.ShapeDtypeStruct((share, hidden), BF16),
            jax.ShapeDtypeStruct((tok_dev, features), BF16),
        ),
        in_specs=[VMEM] * 3,
        out_specs=(HBM, HBM),
        scratch_shapes=[
            pltpu.VMEM((share, hidden), BF16),
            pltpu.VMEM((tok_dev, features), BF16),
            DMA((share // chunk,)),
            DMA,
        ],
        compiler_params=params(),
        cost_estimate=cost(10**9, 4 * 10**6),
        name="finish",
    )(arrived.reshape(n_data * places, share), scaled_all, hits)
    return token_grads[None], weight_grads[None]


def solution(mesh):
    in_specs = (
        P("dp", ("groups", "expert", "tensor"), None),
        P("expert", "dp", "tensor"),
        P("dp", "expert", "groups", "tensor"),
        P("dp", None, "groups"),
        P("dp", None, "groups"),
    )
    out_specs = (
        P("dp", ("groups", "expert", "tensor"), None),
        P(("groups", "expert"), "dp", "tensor"),
    )
    return jax.shard_map(local, mesh=mesh, in_specs=in_specs, out_specs=out_specs, check_vma=False)
```

```python
import functools
import math

import jax
import jax.numpy as jnp
from jax import lax
from jax.experimental import pallas as pl
from jax.experimental.pallas import tpu as pltpu
from jax.sharding import PartitionSpec as P

MOST = 4
BLOCK = 2 * MOST
STRIDE = 11
START = 12
BF16 = jnp.bfloat16
F32 = jnp.float32
VMEM = pl.BlockSpec(memory_space=pltpu.VMEM)
HBM = pl.BlockSpec(memory_space=pltpu.HBM)
DMA = pltpu.SemaphoreType.DMA


def params(limit_mib=24):
    return pltpu.CompilerParams(vmem_limit_bytes=limit_mib * 2**20)


def cost(flops, moved):
    return pl.CostEstimate(flops=flops, bytes_accessed=moved, transcendentals=0)


def exchange_order(n_expert, n_tensor, n_data):
    walk = [
        (d, h, t) for t in range(n_tensor) for h in range(n_expert) for d in reversed(range(n_data))
    ]
    n = len(walk)
    stride = STRIDE if math.gcd(STRIDE, n) == 1 else 1
    return [walk[(stride * k + START) % n] for k in range(n)]


def to_column(row):
    n = row.shape[1]
    eye = lax.broadcasted_iota(jnp.int32, (n, n), 0) == lax.broadcasted_iota(jnp.int32, (n, n), 1)
    return jnp.sum(jnp.where(eye, row, jnp.zeros_like(row)), axis=1, keepdims=True)


def owner_and_arrival(chosen, tok_dev):
    n = chosen.shape[1]
    owner = chosen // tok_dev
    before = lax.broadcasted_iota(jnp.int32, (n, n), 0) < lax.broadcasted_iota(jnp.int32, (n, n), 1)
    same = to_column(owner) == owner
    arrival = jnp.sum(jnp.where(same & before, 1, 0), axis=0, keepdims=True)
    return owner, arrival


def own_places(chosen_ref, gate_ref, slots, owner_id, tok_dev):
    targets, gates = [], []
    for e, (owner, arrival) in enumerate(slots):
        chosen = chosen_ref[e : e + 1, :]
        place = jnp.where(owner == owner_id, arrival, -1)
        hit = lax.broadcasted_iota(jnp.int32, (MOST, chosen.shape[1]), 0) == place
        targets.append(jnp.sum(jnp.where(hit, chosen - owner * tok_dev + 1, 0), axis=1, keepdims=True))
        gates.append(jnp.sum(jnp.where(hit, gate_ref[e : e + 1, :], 0.0), axis=1, keepdims=True))
    return targets, gates


def as_onehot(mask):
    return mask.astype(F32).astype(BF16)


def block_of(order, owner, group, n_tensor):
    out = jnp.zeros_like(owner)
    for k, (d, h, t) in enumerate(order):
        out = out + jnp.where((owner == h * n_tensor + t) & (group == d), k, 0)
    return out


def spread(place, blocks):
    return as_onehot(lax.broadcasted_iota(jnp.int32, (blocks * BLOCK, place.shape[1]), 0) == place)


def prep_kernel(
    order,
    n_expert,
    n_tensor,
    n_data,
    chosen_hbm,
    gate_hbm,
    grads_hbm,
    tokens_hbm,
    send_ref,
    grads_ref,
    placed_ref,
    place_ref,
    hits_ref,
    chosen_ref,
    gate_ref,
    tokens_ref,
    sems,
):
    pairs = (
        (chosen_hbm, chosen_ref),
        (gate_hbm, gate_ref),
        (grads_hbm, grads_ref),
        (tokens_hbm, tokens_ref),
    )
    loads = [pltpu.make_async_copy(src, dst, sems.at[i]) for i, (src, dst) in enumerate(pairs)]
    for load in loads:
        load.start()
    tok_dev, features = tokens_ref.shape
    experts = chosen_ref.shape[0]
    halves = n_expert // experts
    blocks = len(order)
    share = features // n_data
    own_half = lax.axis_index("expert")
    owner_id = own_half * n_tensor + lax.axis_index("tensor")
    own_expert = own_half // halves
    group = lax.axis_index("dp")
    loads[0].wait()
    loads[1].wait()
    slots = [owner_and_arrival(chosen_ref[e : e + 1, :], tok_dev) for e in range(experts)]
    owner = sum(jnp.where(own_expert == e, slot[0], 0) for e, slot in enumerate(slots))
    arrival = sum(jnp.where(own_expert == e, slot[1], 0) for e, slot in enumerate(slots))
    place = block_of(order, owner, group, n_tensor) * BLOCK + arrival
    place_ref[...] = place
    targets, gates = own_places(chosen_ref, gate_ref, slots, owner_id, tok_dev)
    none, no_gate = jnp.zeros_like(targets[0]), jnp.zeros_like(gates[0])
    rows = lax.broadcasted_iota(jnp.int32, (blocks * BLOCK, tok_dev), 1) + 1
    for side in range(n_data):
        ours = [h // halves if d == side else None for d, h, t in order]
        target = jnp.concatenate([p for e in ours for p in (none, none if e is None else targets[e])], axis=0)
        gate = jnp.concatenate([p for e in ours for p in (no_gate, no_gate if e is None else gates[e])], axis=0)
        weighted = jnp.where(rows == target, gate, 0.0)
        high = weighted.astype(BF16)
        hits_ref[side, 0] = high
        hits_ref[side, 1] = (weighted - high.astype(F32)).astype(BF16)
    rows = lax.broadcasted_iota(jnp.int32, (experts * BLOCK, tok_dev), 1) + 1
    pick = as_onehot(rows == jnp.concatenate([p for target in targets for p in (target, none)], axis=0))
    gate = jnp.concatenate([p for g in gates for p in (g, no_gate)], axis=0)
    loads[2].wait()
    placed_ref[...] = jnp.dot(spread(place, blocks), grads_ref[...], preferred_element_type=F32).astype(BF16)
    loads[3].wait()
    picked = gate * jnp.dot(pick, tokens_ref[...], preferred_element_type=F32)
    for k, (d, h, t) in enumerate(order):
        e = h // halves
        send_ref[k * BLOCK : (k + 1) * BLOCK, :] = picked[
            e * BLOCK : (e + 1) * BLOCK, d * share : (d + 1) * share
        ].astype(BF16)


def partial_kernel(
    order,
    n_expert,
    n_tensor,
    tok_dev,
    chosen_ref,
    other_ref,
    weight_ref,
    rows_ref,
    grads_ref,
    placed_ref,
    place_ref,
    send_ref,
    all_ref,
):
    blocks = len(order)
    halves = n_expert // chosen_ref.shape[0]
    capacity = chosen_ref.shape[1]
    own_expert = lax.axis_index("expert") // halves
    owner, arrival = owner_and_arrival(chosen_ref[pl.ds(own_expert, 1), :], tok_dev)
    place = block_of(order, owner, 1 - lax.axis_index("dp"), n_tensor) * BLOCK + arrival
    other = other_ref[...]
    part = lax.dot_general(
        jnp.concatenate([grads_ref[...], other], axis=0),
        weight_ref[...],
        (((1,), (1,)), ((), ())),
        preferred_element_type=F32,
    ).astype(BF16)
    out = rows_ref[...].astype(F32)
    for put, piece in ((place_ref[...], part[:capacity]), (place, part[capacity:])):
        out = out + jnp.dot(spread(put + MOST, blocks), piece, preferred_element_type=F32)
    send_ref[...] = out.astype(BF16)
    theirs = jnp.dot(spread(place, blocks), other, preferred_element_type=F32)
    all_ref[...] = (placed_ref[...].astype(F32) + theirs).astype(BF16)


def finish_kernel(
    n_data, chunk, arrived_ref, scaled_ref, hits_ref, weight_hbm, token_hbm, weight_buf, token_buf, weight_sems, token_sem
):
    share, hidden = weight_hbm.shape
    stores = []
    for i in range(share // chunk):
        here = slice(i * chunk, (i + 1) * chunk)
        weight_buf[here, :] = lax.dot_general(
            arrived_ref[:, here], scaled_ref[...], (((0,), (0,)), ((), ())), preferred_element_type=F32
        ).astype(BF16)
        stores.append(pltpu.make_async_copy(weight_buf.at[here, :], weight_hbm.at[here, :], weight_sems.at[i]))
        stores[-1].start()
    for d in range(n_data):
        total = sum(
            lax.dot_general(hits_ref[d, i], arrived_ref[...], (((0,), (0,)), ((), ())), preferred_element_type=F32)
            for i in range(2)
        )
        token_buf[:, d * share : (d + 1) * share] = total.astype(BF16)
    stores.append(pltpu.make_async_copy(token_buf, token_hbm, token_sem))
    stores[-1].start()
    for store in stores:
        store.wait()


def local(tokens, proj_weight, slot_grads, gate_weights, selected):
    n_tensor = lax.axis_size("tensor")
    n_expert = lax.axis_size("expert")
    n_data = lax.axis_size("dp")
    order = exchange_order(n_expert, n_tensor, n_data)
    members = len(order)
    tok_dev, features = tokens.shape[1:]
    hidden = proj_weight.shape[2]
    experts, capacity = selected.shape[1:]
    share = features // n_data
    chosen, gate, grads = selected[0], gate_weights[0], slot_grads[0, 0]
    swap = [(0, 1), (1, 0)]
    other_grads = lax.ppermute(grads, "dp", swap)
    other_chosen = lax.ppermute(chosen, "dp", swap)
    rows, own_grads, placed, place, hits = pl.pallas_call(
        functools.partial(prep_kernel, order, n_expert, n_tensor, n_data),
        out_shape=(
            jax.ShapeDtypeStruct((members * BLOCK, share), BF16),
            jax.ShapeDtypeStruct((capacity, hidden), BF16),
            jax.ShapeDtypeStruct((members * BLOCK, hidden), BF16),
            jax.ShapeDtypeStruct((1, capacity), jnp.int32),
            jax.ShapeDtypeStruct((n_data, 2, members * BLOCK, tok_dev), BF16),
        ),
        in_specs=[HBM] * 4,
        out_specs=(VMEM,) * 5,
        scratch_shapes=[
            pltpu.VMEM((experts, capacity), jnp.int32),
            pltpu.VMEM((experts, capacity), F32),
            pltpu.VMEM((tok_dev, features), BF16),
            DMA((4,)),
        ],
        compiler_params=params(),
        cost_estimate=cost(12 * 10**8, 10**6),
        name="prep",
    )(*(pltpu.with_memory_space_constraint(x, pltpu.HBM) for x in (chosen, gate, grads, tokens[0])))
    send, scaled_all = pl.pallas_call(
        functools.partial(partial_kernel, order, n_expert, n_tensor, tok_dev),
        out_shape=(
            jax.ShapeDtypeStruct((members * BLOCK, share), BF16),
            jax.ShapeDtypeStruct((members * BLOCK, hidden), BF16),
        ),
        in_specs=[VMEM] * 7,
        out_specs=(VMEM, VMEM),
        compiler_params=params(),
        cost_estimate=cost(10**9, 4 * 10**6),
        name="partial",
    )(other_chosen, other_grads, proj_weight[0], rows, own_grads, placed, place)
    arrived = lax.all_to_all(
        send.reshape(members, BLOCK, share),
        ("expert", "dp", "tensor"),
        split_axis=0,
        concat_axis=0,
        tiled=True,
        axis_index_groups=[[(h * n_data + d) * n_tensor + t for d, h, t in order]],
    )
    chunk = min(128, share)
    weight_grads, token_grads = pl.pallas_call(
        functools.partial(finish_kernel, n_data, chunk),
        out_shape=(
            jax.ShapeDtypeStruct((share, hidden), BF16),
            jax.ShapeDtypeStruct((tok_dev, features), BF16),
        ),
        in_specs=[VMEM] * 3,
        out_specs=(HBM, HBM),
        scratch_shapes=[
            pltpu.VMEM((share, hidden), BF16),
            pltpu.VMEM((tok_dev, features), BF16),
            DMA((share // chunk,)),
            DMA,
        ],
        compiler_params=params(),
        cost_estimate=cost(10**9, 4 * 10**6),
        name="finish",
    )(arrived.reshape(members * BLOCK, share), scaled_all, hits)
    return token_grads[None], weight_grads[None]


def solution(mesh):
    in_specs = (
        P("dp", ("groups", "expert", "tensor"), None),
        P("expert", "dp", "tensor"),
        P("dp", "expert", "groups", "tensor"),
        P("dp", None, "groups"),
        P("dp", None, "groups"),
    )
    out_specs = (
        P("dp", ("groups", "expert", "tensor"), None),
        P(("groups", "expert"), "dp", "tensor"),
    )
    return jax.shard_map(local, mesh=mesh, in_specs=in_specs, out_specs=out_specs, check_vma=False)
```

```python
import functools
import math

import jax
import jax.numpy as jnp
from jax import lax
from jax.experimental import pallas as pl
from jax.experimental.pallas import tpu as pltpu
from jax.sharding import PartitionSpec as P

MOST = 4
BLOCK = 2 * MOST
STRIDE = 11
START = 12
EARLIER = 3
LATER = 7
BF16 = jnp.bfloat16
F32 = jnp.float32
VMEM = pl.BlockSpec(memory_space=pltpu.VMEM)
HBM = pl.BlockSpec(memory_space=pltpu.HBM)
DMA = pltpu.SemaphoreType.DMA


def params(limit_mib=24):
    return pltpu.CompilerParams(vmem_limit_bytes=limit_mib * 2**20)


def cost(flops, moved):
    return pl.CostEstimate(flops=flops, bytes_accessed=moved, transcendentals=0)


def exchange_order(n_expert, n_tensor, n_data):
    walk = [
        (d, h, t) for t in range(n_tensor) for h in range(n_expert) for d in reversed(range(n_data))
    ]
    n = len(walk)
    stride = STRIDE if math.gcd(STRIDE, n) == 1 else 1
    order = [walk[(stride * k + START) % n] for k in range(n)]
    order.insert(LATER % n, order.pop(EARLIER % n))
    return order


def to_column(row):
    n = row.shape[1]
    eye = lax.broadcasted_iota(jnp.int32, (n, n), 0) == lax.broadcasted_iota(jnp.int32, (n, n), 1)
    return jnp.sum(jnp.where(eye, row, jnp.zeros_like(row)), axis=1, keepdims=True)


def owner_and_arrival(chosen, tok_dev):
    n = chosen.shape[1]
    owner = chosen // tok_dev
    before = lax.broadcasted_iota(jnp.int32, (n, n), 0) < lax.broadcasted_iota(jnp.int32, (n, n), 1)
    same = to_column(owner) == owner
    arrival = jnp.sum(jnp.where(same & before, 1, 0), axis=0, keepdims=True)
    return owner, arrival


def own_places(chosen_ref, gate_ref, slots, owner_id, tok_dev):
    targets, gates = [], []
    for e, (owner, arrival) in enumerate(slots):
        chosen = chosen_ref[e : e + 1, :]
        place = jnp.where(owner == owner_id, arrival, -1)
        hit = lax.broadcasted_iota(jnp.int32, (MOST, chosen.shape[1]), 0) == place
        targets.append(jnp.sum(jnp.where(hit, chosen - owner * tok_dev + 1, 0), axis=1, keepdims=True))
        gates.append(jnp.sum(jnp.where(hit, gate_ref[e : e + 1, :], 0.0), axis=1, keepdims=True))
    return targets, gates


def as_onehot(mask):
    return mask.astype(F32).astype(BF16)


def block_of(order, owner, group, n_tensor):
    out = jnp.zeros_like(owner)
    for k, (d, h, t) in enumerate(order):
        out = out + jnp.where((owner == h * n_tensor + t) & (group == d), k, 0)
    return out


def spread(place, blocks):
    return as_onehot(lax.broadcasted_iota(jnp.int32, (blocks * BLOCK, place.shape[1]), 0) == place)


def prep_kernel(
    order,
    n_expert,
    n_tensor,
    n_data,
    chosen_hbm,
    gate_hbm,
    grads_hbm,
    tokens_hbm,
    send_ref,
    grads_ref,
    place_ref,
    hits_ref,
    chosen_ref,
    gate_ref,
    tokens_ref,
    sems,
):
    pairs = (
        (chosen_hbm, chosen_ref),
        (gate_hbm, gate_ref),
        (grads_hbm, grads_ref),
        (tokens_hbm, tokens_ref),
    )
    loads = [pltpu.make_async_copy(src, dst, sems.at[i]) for i, (src, dst) in enumerate(pairs)]
    for load in loads:
        load.start()
    tok_dev, features = tokens_ref.shape
    experts = chosen_ref.shape[0]
    halves = n_expert // experts
    blocks = len(order)
    share = features // n_data
    own_half = lax.axis_index("expert")
    owner_id = own_half * n_tensor + lax.axis_index("tensor")
    own_expert = own_half // halves
    group = lax.axis_index("dp")
    loads[0].wait()
    loads[1].wait()
    slots = [owner_and_arrival(chosen_ref[e : e + 1, :], tok_dev) for e in range(experts)]
    owner = sum(jnp.where(own_expert == e, slot[0], 0) for e, slot in enumerate(slots))
    arrival = sum(jnp.where(own_expert == e, slot[1], 0) for e, slot in enumerate(slots))
    place = block_of(order, owner, group, n_tensor) * BLOCK + arrival
    place_ref[...] = place
    targets, gates = own_places(chosen_ref, gate_ref, slots, owner_id, tok_dev)
    none, no_gate = jnp.zeros_like(targets[0]), jnp.zeros_like(gates[0])
    rows = lax.broadcasted_iota(jnp.int32, (blocks * BLOCK, tok_dev), 1) + 1
    for side in range(n_data):
        ours = [h // halves if d == side else None for d, h, t in order]
        target = jnp.concatenate([p for e in ours for p in (none, none if e is None else targets[e])], axis=0)
        gate = jnp.concatenate([p for e in ours for p in (no_gate, no_gate if e is None else gates[e])], axis=0)
        weighted = jnp.where(rows == target, gate, 0.0)
        high = weighted.astype(BF16)
        hits_ref[side, 0] = high
        hits_ref[side, 1] = (weighted - high.astype(F32)).astype(BF16)
    rows = lax.broadcasted_iota(jnp.int32, (experts * BLOCK, tok_dev), 1) + 1
    pick = as_onehot(rows == jnp.concatenate([p for target in targets for p in (target, none)], axis=0))
    gate = jnp.concatenate([p for g in gates for p in (g, no_gate)], axis=0)
    loads[3].wait()
    picked = gate * jnp.dot(pick, tokens_ref[...], preferred_element_type=F32)
    for k, (d, h, t) in enumerate(order):
        e = h // halves
        send_ref[k * BLOCK : (k + 1) * BLOCK, :] = picked[
            e * BLOCK : (e + 1) * BLOCK, d * share : (d + 1) * share
        ].astype(BF16)
    loads[2].wait()


def partial_kernel(
    order,
    n_expert,
    n_tensor,
    tok_dev,
    chosen_ref,
    other_ref,
    weight_ref,
    rows_ref,
    grads_ref,
    place_ref,
    send_ref,
    all_ref,
):
    blocks = len(order)
    halves = n_expert // chosen_ref.shape[0]
    own_expert = lax.axis_index("expert") // halves
    owner, arrival = owner_and_arrival(chosen_ref[pl.ds(own_expert, 1), :], tok_dev)
    other = block_of(order, owner, 1 - lax.axis_index("dp"), n_tensor) * BLOCK + arrival
    place = jnp.concatenate([place_ref[...], other], axis=1)
    grads = jnp.concatenate([grads_ref[...], other_ref[...]], axis=0)
    all_ref[...] = jnp.dot(spread(place, blocks), grads, preferred_element_type=F32).astype(BF16)
    part = lax.dot_general(
        grads, weight_ref[...], (((1,), (1,)), ((), ())), preferred_element_type=F32
    ).astype(BF16)
    out = jnp.dot(spread(place + MOST, blocks), part, preferred_element_type=F32)
    send_ref[...] = (out + rows_ref[...].astype(F32)).astype(BF16)


def finish_kernel(
    n_data, chunk, arrived_ref, scaled_ref, hits_ref, weight_hbm, token_hbm, weight_buf, token_buf, weight_sems, token_sem
):
    share, hidden = weight_hbm.shape
    stores = []
    for i in range(share // chunk):
        here = slice(i * chunk, (i + 1) * chunk)
        weight_buf[here, :] = lax.dot_general(
            arrived_ref[:, here], scaled_ref[...], (((0,), (0,)), ((), ())), preferred_element_type=F32
        ).astype(BF16)
        stores.append(pltpu.make_async_copy(weight_buf.at[here, :], weight_hbm.at[here, :], weight_sems.at[i]))
        stores[-1].start()
    for d in range(n_data):
        total = sum(
            lax.dot_general(hits_ref[d, i], arrived_ref[...], (((0,), (0,)), ((), ())), preferred_element_type=F32)
            for i in range(2)
        )
        token_buf[:, d * share : (d + 1) * share] = total.astype(BF16)
    stores.append(pltpu.make_async_copy(token_buf, token_hbm, token_sem))
    stores[-1].start()
    for store in stores:
        store.wait()


def local(tokens, proj_weight, slot_grads, gate_weights, selected):
    n_tensor = lax.axis_size("tensor")
    n_expert = lax.axis_size("expert")
    n_data = lax.axis_size("dp")
    order = exchange_order(n_expert, n_tensor, n_data)
    members = len(order)
    tok_dev, features = tokens.shape[1:]
    hidden = proj_weight.shape[2]
    experts, capacity = selected.shape[1:]
    share = features // n_data
    chosen, gate, grads = selected[0], gate_weights[0], slot_grads[0, 0]
    swap = [(0, 1), (1, 0)]
    other_grads = lax.ppermute(grads, "dp", swap)
    other_chosen = lax.ppermute(chosen, "dp", swap)
    rows, own_grads, place, hits = pl.pallas_call(
        functools.partial(prep_kernel, order, n_expert, n_tensor, n_data),
        out_shape=(
            jax.ShapeDtypeStruct((members * BLOCK, share), BF16),
            jax.ShapeDtypeStruct((capacity, hidden), BF16),
            jax.ShapeDtypeStruct((1, capacity), jnp.int32),
            jax.ShapeDtypeStruct((n_data, 2, members * BLOCK, tok_dev), BF16),
        ),
        in_specs=[HBM] * 4,
        out_specs=(VMEM,) * 4,
        scratch_shapes=[
            pltpu.VMEM((experts, capacity), jnp.int32),
            pltpu.VMEM((experts, capacity), F32),
            pltpu.VMEM((tok_dev, features), BF16),
            DMA((4,)),
        ],
        compiler_params=params(),
        cost_estimate=cost(12 * 10**8, 10**6),
        name="prep",
    )(*(pltpu.with_memory_space_constraint(x, pltpu.HBM) for x in (chosen, gate, grads, tokens[0])))
    send, scaled_all = pl.pallas_call(
        functools.partial(partial_kernel, order, n_expert, n_tensor, tok_dev),
        out_shape=(
            jax.ShapeDtypeStruct((members * BLOCK, share), BF16),
            jax.ShapeDtypeStruct((members * BLOCK, hidden), BF16),
        ),
        in_specs=[VMEM] * 6,
        out_specs=(VMEM, VMEM),
        compiler_params=params(),
        cost_estimate=cost(10**9, 4 * 10**6),
        name="partial",
    )(other_chosen, other_grads, proj_weight[0], rows, own_grads, place)
    arrived = lax.all_to_all(
        send.reshape(members, BLOCK, share),
        ("expert", "dp", "tensor"),
        split_axis=0,
        concat_axis=0,
        tiled=True,
        axis_index_groups=[[(h * n_data + d) * n_tensor + t for d, h, t in order]],
    )
    chunk = min(128, share)
    weight_grads, token_grads = pl.pallas_call(
        functools.partial(finish_kernel, n_data, chunk),
        out_shape=(
            jax.ShapeDtypeStruct((share, hidden), BF16),
            jax.ShapeDtypeStruct((tok_dev, features), BF16),
        ),
        in_specs=[VMEM] * 3,
        out_specs=(HBM, HBM),
        scratch_shapes=[
            pltpu.VMEM((share, hidden), BF16),
            pltpu.VMEM((tok_dev, features), BF16),
            DMA((share // chunk,)),
            DMA,
        ],
        compiler_params=params(),
        cost_estimate=cost(10**9, 4 * 10**6),
        name="finish",
    )(arrived.reshape(members * BLOCK, share), scaled_all, hits)
    return token_grads[None], weight_grads[None]


def solution(mesh):
    in_specs = (
        P("dp", ("groups", "expert", "tensor"), None),
        P("expert", "dp", "tensor"),
        P("dp", "expert", "groups", "tensor"),
        P("dp", None, "groups"),
        P("dp", None, "groups"),
    )
    out_specs = (
        P("dp", ("groups", "expert", "tensor"), None),
        P(("groups", "expert"), "dp", "tensor"),
    )
    return jax.shard_map(local, mesh=mesh, in_specs=in_specs, out_specs=out_specs, check_vma=False)
```

```python
import functools
import math

import jax
import jax.numpy as jnp
from jax import lax
from jax.experimental import pallas as pl
from jax.experimental.pallas import tpu as pltpu
from jax.sharding import PartitionSpec as P

MOST = 4
BLOCK = 2 * MOST
STRIDE = 11
START = 12
EARLIER = 3
LATER = 7
BF16 = jnp.bfloat16
F32 = jnp.float32
VMEM = pl.BlockSpec(memory_space=pltpu.VMEM)
HBM = pl.BlockSpec(memory_space=pltpu.HBM)
DMA = pltpu.SemaphoreType.DMA


def params(limit_mib=24):
    return pltpu.CompilerParams(vmem_limit_bytes=limit_mib * 2**20)


def cost(flops, moved):
    return pl.CostEstimate(flops=flops, bytes_accessed=moved, transcendentals=0)


def exchange_order(n_expert, n_tensor, n_data):
    walk = [
        (d, h, t) for t in range(n_tensor) for h in range(n_expert) for d in reversed(range(n_data))
    ]
    n = len(walk)
    stride = STRIDE if math.gcd(STRIDE, n) == 1 else 1
    order = [walk[(stride * k + START) % n] for k in range(n)]
    order.insert(LATER % n, order.pop(EARLIER % n))
    return order


def to_column(row):
    n = row.shape[1]
    eye = lax.broadcasted_iota(jnp.int32, (n, n), 0) == lax.broadcasted_iota(jnp.int32, (n, n), 1)
    return jnp.sum(jnp.where(eye, row, jnp.zeros_like(row)), axis=1, keepdims=True)


def owner_and_arrival(chosen, tok_dev):
    n = chosen.shape[1]
    owner = chosen // tok_dev
    before = lax.broadcasted_iota(jnp.int32, (n, n), 0) < lax.broadcasted_iota(jnp.int32, (n, n), 1)
    same = to_column(owner) == owner
    arrival = jnp.sum(jnp.where(same & before, 1, 0), axis=0, keepdims=True)
    return owner, arrival


def own_places(chosen_ref, gate_ref, slots, owner_id, tok_dev):
    targets, gates = [], []
    for e, (owner, arrival) in enumerate(slots):
        chosen = chosen_ref[e : e + 1, :]
        place = jnp.where(owner == owner_id, arrival, -1)
        hit = lax.broadcasted_iota(jnp.int32, (MOST, chosen.shape[1]), 0) == place
        targets.append(jnp.sum(jnp.where(hit, chosen - owner * tok_dev + 1, 0), axis=1, keepdims=True))
        gates.append(jnp.sum(jnp.where(hit, gate_ref[e : e + 1, :], 0.0), axis=1, keepdims=True))
    return targets, gates


def as_onehot(mask):
    return mask.astype(F32).astype(BF16)


def block_of(order, owner, group, n_tensor):
    out = jnp.zeros_like(owner)
    for k, (d, h, t) in enumerate(order):
        out = out + jnp.where((owner == h * n_tensor + t) & (group == d), k, 0)
    return out


def spread(place, blocks):
    return as_onehot(lax.broadcasted_iota(jnp.int32, (blocks * BLOCK, place.shape[1]), 0) == place)


def prep_kernel(
    order,
    n_expert,
    n_tensor,
    n_data,
    chosen_hbm,
    gate_hbm,
    grads_hbm,
    tokens_hbm,
    send_ref,
    grads_ref,
    place_ref,
    hits_ref,
    chosen_ref,
    gate_ref,
    tokens_ref,
    sems,
):
    pairs = (
        (chosen_hbm, chosen_ref),
        (gate_hbm, gate_ref),
        (grads_hbm, grads_ref),
        (tokens_hbm, tokens_ref),
    )
    loads = [pltpu.make_async_copy(src, dst, sems.at[i]) for i, (src, dst) in enumerate(pairs)]
    for load in loads:
        load.start()
    tok_dev, features = tokens_ref.shape
    experts = chosen_ref.shape[0]
    halves = n_expert // experts
    blocks = len(order)
    share = features // n_data
    own_half = lax.axis_index("expert")
    owner_id = own_half * n_tensor + lax.axis_index("tensor")
    own_expert = own_half // halves
    group = lax.axis_index("dp")
    loads[0].wait()
    loads[1].wait()
    slots = [owner_and_arrival(chosen_ref[e : e + 1, :], tok_dev) for e in range(experts)]
    owner = sum(jnp.where(own_expert == e, slot[0], 0) for e, slot in enumerate(slots))
    arrival = sum(jnp.where(own_expert == e, slot[1], 0) for e, slot in enumerate(slots))
    place = block_of(order, owner, group, n_tensor) * BLOCK + arrival
    place_ref[...] = place
    targets, gates = own_places(chosen_ref, gate_ref, slots, owner_id, tok_dev)
    none, no_gate = jnp.zeros_like(targets[0]), jnp.zeros_like(gates[0])
    rows = lax.broadcasted_iota(jnp.int32, (blocks * BLOCK, tok_dev), 1) + 1
    for side in range(n_data):
        ours = [h // halves if d == side else None for d, h, t in order]
        target = jnp.concatenate([p for e in ours for p in (none, none if e is None else targets[e])], axis=0)
        gate = jnp.concatenate([p for e in ours for p in (no_gate, no_gate if e is None else gates[e])], axis=0)
        weighted = jnp.where(rows == target, gate, 0.0)
        high = weighted.astype(BF16)
        hits_ref[side, 0] = high
        hits_ref[side, 1] = (weighted - high.astype(F32)).astype(BF16)
    rows = lax.broadcasted_iota(jnp.int32, (experts * BLOCK, tok_dev), 1) + 1
    pick = as_onehot(rows == jnp.concatenate([p for target in targets for p in (target, none)], axis=0))
    gate = jnp.concatenate([p for g in gates for p in (g, no_gate)], axis=0)
    loads[3].wait()
    picked = gate * jnp.dot(pick, tokens_ref[...], preferred_element_type=F32)
    for k, (d, h, t) in enumerate(order):
        e = h // halves
        send_ref[k * BLOCK : (k + 1) * BLOCK, :] = picked[
            e * BLOCK : (e + 1) * BLOCK, d * share : (d + 1) * share
        ].astype(BF16)
    loads[2].wait()


def partial_kernel(
    order,
    n_expert,
    n_tensor,
    tok_dev,
    chosen_ref,
    other_ref,
    weight_ref,
    rows_ref,
    grads_ref,
    place_ref,
    send_ref,
    all_ref,
):
    blocks = len(order)
    halves = n_expert // chosen_ref.shape[0]
    own_expert = lax.axis_index("expert") // halves
    owner, arrival = owner_and_arrival(chosen_ref[pl.ds(own_expert, 1), :], tok_dev)
    other = block_of(order, owner, 1 - lax.axis_index("dp"), n_tensor) * BLOCK + arrival
    place = jnp.concatenate([place_ref[...], other], axis=1)
    grads = jnp.concatenate([grads_ref[...], other_ref[...]], axis=0)
    part = lax.dot_general(
        grads, weight_ref[...], (((1,), (1,)), ((), ())), preferred_element_type=F32
    ).astype(BF16)
    out = jnp.dot(spread(place + MOST, blocks), part, preferred_element_type=F32)
    send_ref[...] = (out + rows_ref[...].astype(F32)).astype(BF16)
    all_ref[...] = jnp.dot(spread(place, blocks), grads, preferred_element_type=F32).astype(BF16)


def finish_kernel(
    n_data, chunk, arrived_ref, scaled_ref, hits_ref, weight_hbm, token_hbm, weight_buf, token_buf, weight_sems, token_sem
):
    share, hidden = weight_hbm.shape
    stores = []
    for i in range(share // chunk):
        here = slice(i * chunk, (i + 1) * chunk)
        weight_buf[here, :] = lax.dot_general(
            arrived_ref[:, here], scaled_ref[...], (((0,), (0,)), ((), ())), preferred_element_type=F32
        ).astype(BF16)
        stores.append(pltpu.make_async_copy(weight_buf.at[here, :], weight_hbm.at[here, :], weight_sems.at[i]))
        stores[-1].start()
    for d in range(n_data):
        total = sum(
            lax.dot_general(hits_ref[d, i], arrived_ref[...], (((0,), (0,)), ((), ())), preferred_element_type=F32)
            for i in range(2)
        )
        token_buf[:, d * share : (d + 1) * share] = total.astype(BF16)
    stores.append(pltpu.make_async_copy(token_buf, token_hbm, token_sem))
    stores[-1].start()
    for store in stores:
        store.wait()


def local(tokens, proj_weight, slot_grads, gate_weights, selected):
    n_tensor = lax.axis_size("tensor")
    n_expert = lax.axis_size("expert")
    n_data = lax.axis_size("dp")
    order = exchange_order(n_expert, n_tensor, n_data)
    members = len(order)
    tok_dev, features = tokens.shape[1:]
    hidden = proj_weight.shape[2]
    experts, capacity = selected.shape[1:]
    share = features // n_data
    chosen, gate, grads = selected[0], gate_weights[0], slot_grads[0, 0]
    swap = [(0, 1), (1, 0)]
    other_grads = lax.ppermute(grads, "dp", swap)
    other_chosen = lax.ppermute(chosen, "dp", swap)
    rows, own_grads, place, hits = pl.pallas_call(
        functools.partial(prep_kernel, order, n_expert, n_tensor, n_data),
        out_shape=(
            jax.ShapeDtypeStruct((members * BLOCK, share), BF16),
            jax.ShapeDtypeStruct((capacity, hidden), BF16),
            jax.ShapeDtypeStruct((1, capacity), jnp.int32),
            jax.ShapeDtypeStruct((n_data, 2, members * BLOCK, tok_dev), BF16),
        ),
        in_specs=[HBM] * 4,
        out_specs=(VMEM,) * 4,
        scratch_shapes=[
            pltpu.VMEM((experts, capacity), jnp.int32),
            pltpu.VMEM((experts, capacity), F32),
            pltpu.VMEM((tok_dev, features), BF16),
            DMA((4,)),
        ],
        compiler_params=params(),
        cost_estimate=cost(12 * 10**8, 10**6),
        name="prep",
    )(*(pltpu.with_memory_space_constraint(x, pltpu.HBM) for x in (chosen, gate, grads, tokens[0])))
    send, scaled_all = pl.pallas_call(
        functools.partial(partial_kernel, order, n_expert, n_tensor, tok_dev),
        out_shape=(
            jax.ShapeDtypeStruct((members * BLOCK, share), BF16),
            jax.ShapeDtypeStruct((members * BLOCK, hidden), BF16),
        ),
        in_specs=[VMEM] * 6,
        out_specs=(VMEM, VMEM),
        compiler_params=params(),
        cost_estimate=cost(10**9, 4 * 10**6),
        name="partial",
    )(other_chosen, other_grads, proj_weight[0], rows, own_grads, place)
    arrived = lax.all_to_all(
        send.reshape(members, BLOCK, share),
        ("expert", "dp", "tensor"),
        split_axis=0,
        concat_axis=0,
        tiled=True,
        axis_index_groups=[[(h * n_data + d) * n_tensor + t for d, h, t in order]],
    )
    chunk = min(128, share)
    weight_grads, token_grads = pl.pallas_call(
        functools.partial(finish_kernel, n_data, chunk),
        out_shape=(
            jax.ShapeDtypeStruct((share, hidden), BF16),
            jax.ShapeDtypeStruct((tok_dev, features), BF16),
        ),
        in_specs=[VMEM] * 3,
        out_specs=(HBM, HBM),
        scratch_shapes=[
            pltpu.VMEM((share, hidden), BF16),
            pltpu.VMEM((tok_dev, features), BF16),
            DMA((share // chunk,)),
            DMA,
        ],
        compiler_params=params(),
        cost_estimate=cost(10**9, 4 * 10**6),
        name="finish",
    )(arrived.reshape(members * BLOCK, share), scaled_all, hits)
    return token_grads[None], weight_grads[None]


def solution(mesh):
    in_specs = (
        P("dp", ("groups", "expert", "tensor"), None),
        P("expert", "dp", "tensor"),
        P("dp", "expert", "groups", "tensor"),
        P("dp", None, "groups"),
        P("dp", None, "groups"),
    )
    out_specs = (
        P("dp", ("groups", "expert", "tensor"), None),
        P(("groups", "expert"), "dp", "tensor"),
    )
    return jax.shard_map(local, mesh=mesh, in_specs=in_specs, out_specs=out_specs, check_vma=False)
```

```python
import functools
import math

import jax
import jax.numpy as jnp
from jax import lax
from jax.experimental import pallas as pl
from jax.experimental.pallas import tpu as pltpu
from jax.sharding import PartitionSpec as P

MOST = 4
BLOCK = 2 * MOST
STRIDE = 11
START = 12
EARLIER = 3
LATER = 7
EXCHANGED = ((6, 10), (8, 14))
BF16 = jnp.bfloat16
F32 = jnp.float32
VMEM = pl.BlockSpec(memory_space=pltpu.VMEM)
HBM = pl.BlockSpec(memory_space=pltpu.HBM)
DMA = pltpu.SemaphoreType.DMA


def params(limit_mib=24):
    return pltpu.CompilerParams(vmem_limit_bytes=limit_mib * 2**20)


def cost(flops, moved):
    return pl.CostEstimate(flops=flops, bytes_accessed=moved, transcendentals=0)


def exchange_order(n_expert, n_tensor, n_data):
    walk = [
        (d, h, t) for t in range(n_tensor) for h in range(n_expert) for d in reversed(range(n_data))
    ]
    n = len(walk)
    stride = STRIDE if math.gcd(STRIDE, n) == 1 else 1
    order = [walk[(stride * k + START) % n] for k in range(n)]
    order.insert(LATER % n, order.pop(EARLIER % n))
    for i, j in EXCHANGED:
        order[i % n], order[j % n] = order[j % n], order[i % n]
    return order


def to_column(row):
    n = row.shape[1]
    eye = lax.broadcasted_iota(jnp.int32, (n, n), 0) == lax.broadcasted_iota(jnp.int32, (n, n), 1)
    return jnp.sum(jnp.where(eye, row, jnp.zeros_like(row)), axis=1, keepdims=True)


def owner_and_arrival(chosen, tok_dev):
    n = chosen.shape[1]
    owner = chosen // tok_dev
    before = lax.broadcasted_iota(jnp.int32, (n, n), 0) < lax.broadcasted_iota(jnp.int32, (n, n), 1)
    same = to_column(owner) == owner
    arrival = jnp.sum(jnp.where(same & before, 1, 0), axis=0, keepdims=True)
    return owner, arrival


def own_places(chosen_ref, gate_ref, slots, owner_id, tok_dev):
    targets, gates = [], []
    for e, (owner, arrival) in enumerate(slots):
        chosen = chosen_ref[e : e + 1, :]
        place = jnp.where(owner == owner_id, arrival, -1)
        hit = lax.broadcasted_iota(jnp.int32, (MOST, chosen.shape[1]), 0) == place
        targets.append(jnp.sum(jnp.where(hit, chosen - owner * tok_dev + 1, 0), axis=1, keepdims=True))
        gates.append(jnp.sum(jnp.where(hit, gate_ref[e : e + 1, :], 0.0), axis=1, keepdims=True))
    return targets, gates


def as_onehot(mask):
    return mask.astype(F32).astype(BF16)


def block_of(order, owner, group, n_tensor):
    out = jnp.zeros_like(owner)
    for k, (d, h, t) in enumerate(order):
        out = out + jnp.where((owner == h * n_tensor + t) & (group == d), k, 0)
    return out


def spread(place, blocks):
    return as_onehot(lax.broadcasted_iota(jnp.int32, (blocks * BLOCK, place.shape[1]), 0) == place)


def prep_kernel(
    order,
    n_expert,
    n_tensor,
    n_data,
    chosen_hbm,
    gate_hbm,
    grads_hbm,
    tokens_hbm,
    send_ref,
    grads_ref,
    place_ref,
    hits_ref,
    chosen_ref,
    gate_ref,
    tokens_ref,
    sems,
):
    pairs = (
        (chosen_hbm, chosen_ref),
        (gate_hbm, gate_ref),
        (grads_hbm, grads_ref),
        (tokens_hbm, tokens_ref),
    )
    loads = [pltpu.make_async_copy(src, dst, sems.at[i]) for i, (src, dst) in enumerate(pairs)]
    for load in loads:
        load.start()
    tok_dev, features = tokens_ref.shape
    experts = chosen_ref.shape[0]
    halves = n_expert // experts
    blocks = len(order)
    share = features // n_data
    own_half = lax.axis_index("expert")
    owner_id = own_half * n_tensor + lax.axis_index("tensor")
    own_expert = own_half // halves
    group = lax.axis_index("dp")
    loads[0].wait()
    loads[1].wait()
    slots = [owner_and_arrival(chosen_ref[e : e + 1, :], tok_dev) for e in range(experts)]
    owner = sum(jnp.where(own_expert == e, slot[0], 0) for e, slot in enumerate(slots))
    arrival = sum(jnp.where(own_expert == e, slot[1], 0) for e, slot in enumerate(slots))
    place = block_of(order, owner, group, n_tensor) * BLOCK + arrival
    place_ref[...] = place
    targets, gates = own_places(chosen_ref, gate_ref, slots, owner_id, tok_dev)
    none, no_gate = jnp.zeros_like(targets[0]), jnp.zeros_like(gates[0])
    rows = lax.broadcasted_iota(jnp.int32, (experts * BLOCK, tok_dev), 1) + 1
    pick = as_onehot(rows == jnp.concatenate([p for target in targets for p in (target, none)], axis=0))
    gate = jnp.concatenate([p for g in gates for p in (g, no_gate)], axis=0)
    loads[3].wait()
    picked = gate * jnp.dot(pick, tokens_ref[...], preferred_element_type=F32)
    for k, (d, h, t) in enumerate(order):
        e = h // halves
        send_ref[k * BLOCK : (k + 1) * BLOCK, :] = picked[
            e * BLOCK : (e + 1) * BLOCK, d * share : (d + 1) * share
        ].astype(BF16)
    rows = lax.broadcasted_iota(jnp.int32, (blocks * BLOCK, tok_dev), 1) + 1
    for side in range(n_data):
        ours = [h // halves if d == side else None for d, h, t in order]
        target = jnp.concatenate([p for e in ours for p in (none, none if e is None else targets[e])], axis=0)
        gate = jnp.concatenate([p for e in ours for p in (no_gate, no_gate if e is None else gates[e])], axis=0)
        weighted = jnp.where(rows == target, gate, 0.0)
        high = weighted.astype(BF16)
        hits_ref[side, 0] = high
        hits_ref[side, 1] = (weighted - high.astype(F32)).astype(BF16)
    loads[2].wait()


def partial_kernel(
    order,
    n_expert,
    n_tensor,
    tok_dev,
    chosen_ref,
    other_ref,
    weight_ref,
    rows_ref,
    grads_ref,
    place_ref,
    send_ref,
    all_ref,
):
    blocks = len(order)
    halves = n_expert // chosen_ref.shape[0]
    own_expert = lax.axis_index("expert") // halves
    owner, arrival = owner_and_arrival(chosen_ref[pl.ds(own_expert, 1), :], tok_dev)
    other = block_of(order, owner, 1 - lax.axis_index("dp"), n_tensor) * BLOCK + arrival
    place = jnp.concatenate([place_ref[...], other], axis=1)
    grads = jnp.concatenate([grads_ref[...], other_ref[...]], axis=0)
    part = lax.dot_general(
        grads, weight_ref[...], (((1,), (1,)), ((), ())), preferred_element_type=F32
    ).astype(BF16)
    out = jnp.dot(spread(place + MOST, blocks), part, preferred_element_type=F32)
    send_ref[...] = (out + rows_ref[...].astype(F32)).astype(BF16)
    all_ref[...] = jnp.dot(spread(place, blocks), grads, preferred_element_type=F32).astype(BF16)


def finish_kernel(
    n_data, chunk, arrived_ref, scaled_ref, hits_ref, weight_hbm, token_hbm, weight_buf, token_buf, weight_sems, token_sem
):
    share, hidden = weight_hbm.shape
    stores = []
    for i in range(share // chunk):
        here = slice(i * chunk, (i + 1) * chunk)
        weight_buf[here, :] = lax.dot_general(
            arrived_ref[:, here], scaled_ref[...], (((0,), (0,)), ((), ())), preferred_element_type=F32
        ).astype(BF16)
        stores.append(pltpu.make_async_copy(weight_buf.at[here, :], weight_hbm.at[here, :], weight_sems.at[i]))
        stores[-1].start()
    for d in range(n_data):
        total = sum(
            lax.dot_general(hits_ref[d, i], arrived_ref[...], (((0,), (0,)), ((), ())), preferred_element_type=F32)
            for i in range(2)
        )
        token_buf[:, d * share : (d + 1) * share] = total.astype(BF16)
    stores.append(pltpu.make_async_copy(token_buf, token_hbm, token_sem))
    stores[-1].start()
    for store in stores:
        store.wait()


def local(tokens, proj_weight, slot_grads, gate_weights, selected):
    n_tensor = lax.axis_size("tensor")
    n_expert = lax.axis_size("expert")
    n_data = lax.axis_size("dp")
    order = exchange_order(n_expert, n_tensor, n_data)
    members = len(order)
    tok_dev, features = tokens.shape[1:]
    hidden = proj_weight.shape[2]
    experts, capacity = selected.shape[1:]
    share = features // n_data
    chosen, gate, grads = selected[0], gate_weights[0], slot_grads[0, 0]
    swap = [(0, 1), (1, 0)]
    other_grads = lax.ppermute(grads, "dp", swap)
    other_chosen = lax.ppermute(chosen, "dp", swap)
    rows, own_grads, place, hits = pl.pallas_call(
        functools.partial(prep_kernel, order, n_expert, n_tensor, n_data),
        out_shape=(
            jax.ShapeDtypeStruct((members * BLOCK, share), BF16),
            jax.ShapeDtypeStruct((capacity, hidden), BF16),
            jax.ShapeDtypeStruct((1, capacity), jnp.int32),
            jax.ShapeDtypeStruct((n_data, 2, members * BLOCK, tok_dev), BF16),
        ),
        in_specs=[HBM] * 4,
        out_specs=(VMEM,) * 4,
        scratch_shapes=[
            pltpu.VMEM((experts, capacity), jnp.int32),
            pltpu.VMEM((experts, capacity), F32),
            pltpu.VMEM((tok_dev, features), BF16),
            DMA((4,)),
        ],
        compiler_params=params(),
        cost_estimate=cost(12 * 10**8, 10**6),
        name="prep",
    )(*(pltpu.with_memory_space_constraint(x, pltpu.HBM) for x in (chosen, gate, grads, tokens[0])))
    send, scaled_all = pl.pallas_call(
        functools.partial(partial_kernel, order, n_expert, n_tensor, tok_dev),
        out_shape=(
            jax.ShapeDtypeStruct((members * BLOCK, share), BF16),
            jax.ShapeDtypeStruct((members * BLOCK, hidden), BF16),
        ),
        in_specs=[VMEM] * 6,
        out_specs=(VMEM, VMEM),
        compiler_params=params(),
        cost_estimate=cost(10**9, 4 * 10**6),
        name="partial",
    )(other_chosen, other_grads, proj_weight[0], rows, own_grads, place)
    arrived = lax.all_to_all(
        send.reshape(members, BLOCK, share),
        ("expert", "dp", "tensor"),
        split_axis=0,
        concat_axis=0,
        tiled=True,
        axis_index_groups=[[(h * n_data + d) * n_tensor + t for d, h, t in order]],
    )
    chunk = min(128, share)
    weight_grads, token_grads = pl.pallas_call(
        functools.partial(finish_kernel, n_data, chunk),
        out_shape=(
            jax.ShapeDtypeStruct((share, hidden), BF16),
            jax.ShapeDtypeStruct((tok_dev, features), BF16),
        ),
        in_specs=[VMEM] * 3,
        out_specs=(HBM, HBM),
        scratch_shapes=[
            pltpu.VMEM((share, hidden), BF16),
            pltpu.VMEM((tok_dev, features), BF16),
            DMA((share // chunk,)),
            DMA,
        ],
        compiler_params=params(),
        cost_estimate=cost(10**9, 4 * 10**6),
        name="finish",
    )(arrived.reshape(members * BLOCK, share), scaled_all, hits)
    return token_grads[None], weight_grads[None]


def solution(mesh):
    in_specs = (
        P("dp", ("groups", "expert", "tensor"), None),
        P("expert", "dp", "tensor"),
        P("dp", "expert", "groups", "tensor"),
        P("dp", None, "groups"),
        P("dp", None, "groups"),
    )
    out_specs = (
        P("dp", ("groups", "expert", "tensor"), None),
        P(("groups", "expert"), "dp", "tensor"),
    )
    return jax.shard_map(local, mesh=mesh, in_specs=in_specs, out_specs=out_specs, check_vma=False)
```
